1024 devices in a mesh: seq: 16 (over y, core), tp: 8 (over z), dp: 8 (over x).
Axes of the slice: x: 8, y: 8, z: 8, core: 2. Of those that a mesh axis runs over, the one named last changes fastest.
Arguments:
- queries: bfloat16 [32768, 4096], P(('dp', 'seq'), 'tp'), parts along dimension 0, may hold values from -36 to 36
- key_rows: bfloat16 [32768, 4096], P(('dp', 'seq'), 'tp'), parts along dimension 0, may hold values from -36 to 36
- values: bfloat16 [32768, 4096], P(('dp', 'seq'), 'tp'), parts along dimension 0, may hold values from -6 to 6
- modality: int32 [32768], P(('dp', 'seq')), parts along dimension 0, may hold values from 0 to 1, as said below
- out_weight: bfloat16 [2, 4096, 4096], P(None, 'tp'), may hold values from -0.125 to 0.125
Outputs:
- layer_out: bfloat16 [32768, 4096], P(('dp', 'seq'), 'tp'), parts along dimension 0
The draws below stay inside these ranges and needn't reach their ends.
There are 8 independent parts, one for each index of `dp`. The reference program is written for one: setup_inputs(seed, part) draws one part's arguments, and reference() takes and returns one part's arrays. A program takes and returns all parts, laid end to end along the dimension named above; an argument that names none is the same for every part. Nothing has to cross between parts.
Inputs may be any that keep to these rules, and one draw needn't show every extreme that they name: `modality`: 1 marks an image token, 0 a text token.
All inputs are finite; a program needn't handle non-finite values.
Results may differ from the reference program's by a relative error of at most 0.013.
Values may be sent and summed in bfloat16 or wider, within the bound.
A program may use at most 64 MiB of HBM per device.

```python
import jax
import jax.numpy as jnp
from jax import lax

D = 4096
H = 32
HD = 128
TOK_DEV = 256
TOKENS = 4096
N_TP = 8


def rough_field(key):
    base = jax.random.truncated_normal(jax.random.fold_in(key, 3), -4.0, 4.0, (TOKENS, H * HD), jnp.float32) * 1.5
    return base.astype(jnp.bfloat16)


def draw_queries(key, part):
    return rough_field(jax.random.fold_in(key, 41))


def draw_key_rows(key, part):
    return rough_field(jax.random.fold_in(key, 42))


def draw_modality(key, part):
    span_count = max(2, TOKENS // 512)
    starts = jax.random.randint(jax.random.fold_in(key, 21), (span_count,), 0, TOKENS)
    widths = jax.random.randint(jax.random.fold_in(key, 22), (span_count,), 1, max(2, 2 * TOK_DEV))
    positions = jnp.arange(TOKENS, dtype=jnp.int32)
    inside = (positions[:, None] >= starts[None, :]) & (positions[:, None] < starts[None, :] + widths[None, :])
    return jnp.any(inside, axis=1).astype(jnp.int32)


def strengthened(result, rng, source, target, blocks, factor):
    def block_of(axis_at):
        return (jnp.arange(result.shape[axis_at]) // (result.shape[axis_at] // blocks)).reshape((-1,) + (1,) * (result.ndim - 1 - axis_at))

    one_side = jax.random.permutation(rng, blocks)[block_of(target)]
    far = (block_of(target) + blocks // 2) % blocks
    return jnp.where((block_of(source) == one_side) | (block_of(source) == far), factor * result, result)


def shard_levels(stream_key, extent, shards, smallest, high):
    gain = 1.0
    for position, shards_of in shards:
        draws = jax.random.uniform(jax.random.fold_in(jax.random.fold_in(stream_key, 6), position), (shards_of,), jnp.float32, smallest / len(shards), high / len(shards))
        gain = gain * jnp.repeat(jnp.exp(draws), extent[position] // shards_of).reshape((-1,) + (1,) * (len(extent) - 1 - position))
    return gain


def centred(rng, extent, spread, limit, pieces=(), held_as=jnp.bfloat16):
    level = shard_levels(rng, extent, pieces, -0.22, 0.18) if pieces else 1.0
    entries = jax.random.normal(rng, extent, jnp.float32) * spread * level
    return jnp.minimum(jnp.maximum(entries, -limit), limit).astype(held_as)


def bell_draw_with(stream_key, extent, spread, bound, pieces, heavy, held_as=jnp.bfloat16):
    result = spread * jax.random.normal(stream_key, extent, jnp.float32)
    if pieces:
        result = result * shard_levels(stream_key, extent, pieces, -0.22, 0.18)
    return jnp.clip(strengthened(result, jax.random.fold_in(stream_key, 3), *heavy), -bound, bound).astype(held_as)


def setup_inputs(seed: int = 0, part: int = 0) -> dict:
    splits = jax.random.split(jax.random.key(seed), 6)
    part_keys = jax.random.split(jax.random.fold_in(splits[5], part), 6)
    queries = draw_queries(jax.random.fold_in(jax.random.fold_in(splits[5], part), 71), part)
    key_rows = draw_key_rows(jax.random.fold_in(jax.random.fold_in(splits[5], part), 71), part)
    values = centred(part_keys[2], (TOKENS, H * HD), 1.0, 6.0, ((0, 16), (1, 8)))
    modality = draw_modality(jax.random.fold_in(jax.random.fold_in(splits[5], part), 71), part)
    out_weight = bell_draw_with(splits[4], (2, H * HD, D), (H * HD) ** -0.5, 0.125, ((1, 8),), (1, 2, 8, 2.0))
    return dict(queries=queries, key_rows=key_rows, values=values, modality=modality, out_weight=out_weight)


def split_heads(field):
    return field.reshape(TOKENS, H, HD).transpose(1, 0, 2)


def reference(queries, key_rows, values, modality, out_weight):
    score_scale = HD ** -0.5
    positions = jnp.arange(TOKENS, dtype=jnp.int32)
    allowed = positions[:, None] >= positions[None, :]

    def one_head(inputs):
        query_head, key_head, value_head = inputs
        scores = jnp.dot(query_head, key_head.T, preferred_element_type=jnp.float32) * score_scale
        scores = jnp.where(allowed, scores, -jnp.inf)
        largest = jnp.max(scores, axis=1, keepdims=True)
        weights = jnp.exp(scores - largest)
        probabilities = (weights / jnp.sum(weights, axis=1, keepdims=True)).astype(jnp.bfloat16)
        return jnp.dot(probabilities, value_head, preferred_element_type=jnp.float32).astype(jnp.bfloat16)

    attended = lax.map(one_head, (split_heads(queries), split_heads(key_rows), split_heads(values)))
    attended = attended.transpose(1, 0, 2).reshape(TOKENS, H * HD)
    shard_cols = (H // N_TP) * HD
    image_rows = modality[:, None] == 1
    total = jnp.zeros((TOKENS, D), jnp.float32)
    for shard_index in range(N_TP):
        lower = shard_index * shard_cols
        piece = attended[:, lower:lower + shard_cols]
        text_part = jnp.dot(piece, out_weight[0, lower:lower + shard_cols], preferred_element_type=jnp.float32)
        image_part = jnp.dot(piece, out_weight[1, lower:lower + shard_cols], preferred_element_type=jnp.float32)
        partial_value = jnp.where(image_rows, image_part, text_part).astype(jnp.bfloat16)
        total = total + partial_value.astype(jnp.float32)
    return total.astype(jnp.bfloat16)
```

```python
import functools

import jax
import jax.numpy as jnp
from jax import lax
from jax.experimental import pallas as pl
from jax.experimental.pallas import tpu as pltpu
from jax.sharding import PartitionSpec as P

HD = 128
N_TP = 8
MESH = pl.DeviceIdType.MESH
LOG2E = 1.4426950408889634


def fused(
    q_hbm, k_hbm, v_hbm, mod_ref, w_hbm, out_ref,
    qbuf, kbuf, vbuf, mbuf, acc, obuf, abuf, acat, wbuf, psum, rsnd, rrcv,
    local_sem, ksem, vsem, qsem, asem, rsem, q_send, kv_send, fwd_send, rel_send, o_send, r_send,
):
    me = lax.axis_index("seq")
    z = lax.axis_index("tp")
    rows = q_hbm.shape[0]
    half = rows // 2
    cols = out_ref.shape[1]
    y = me // 2
    c = me % 2
    side = y % 2
    out_dir = 2 * side - 1
    head = y // 2
    twin = 1 - 2 * c + me
    mate_chip = y - out_dir
    mate = mate_chip * 2 + c
    factor = HD ** (-0.5) * LOG2E

    def chip(t):
        return lax.rem(t + 16, 8)

    def send(src, dst, ssem, rsem_, seq):
        copy = pltpu.make_async_remote_copy(
            src_ref=src, dst_ref=dst, send_sem=ssem, recv_sem=rsem_,
            device_id={"seq": seq}, device_id_type=MESH,
        )
        return copy

    def k_at(slot):
        return kbuf.at[slot]

    def v_at(slot):
        return vbuf.at[slot, :, pl.ds(0, HD)]

    def head_cols(ref, h):
        return ref.at[:, pl.ds(pl.multiple_of(h * HD, HD), HD)]

    def await_kv(slot):
        send(k_at(slot), k_at(slot), local_sem.at[0], ksem.at[slot], twin).wait_recv()
        send(v_at(slot), v_at(slot), local_sem.at[0], vsem.at[slot], twin).wait_recv()

    own = [
        pltpu.make_async_copy(head_cols(k_hbm, head), k_at(me), ksem.at[me]),
        pltpu.make_async_copy(head_cols(v_hbm, head), v_at(me), vsem.at[me]),
        pltpu.make_async_copy(
            q_hbm.at[pl.ds(pl.multiple_of(c * half, half), half), pl.ds(pl.multiple_of(head * HD, HD), HD)],
            qbuf.at[0, pl.ds(pl.multiple_of(c * half, half), half), :],
            qsem.at[0, c],
        ),
    ]
    for copy in own:
        copy.start()
    w_copy = pltpu.make_async_copy(w_hbm, wbuf, local_sem.at[1])
    w_copy.start()

    barrier = pltpu.get_barrier_semaphore()
    left, right = lax.rem(z + N_TP - 1, N_TP), lax.rem(z + 1, N_TP)
    peers = 0
    for step in (1, 2, 3, -1, -2):
        for core in range(2):
            pl.semaphore_signal(
                barrier, inc=1, device_id={"seq": chip(y + out_dir * step) * 2 + core}, device_id_type=MESH
            )
            peers += 1
    pl.semaphore_signal(barrier, inc=1, device_id={"seq": twin}, device_id_type=MESH)
    for neighbour in (left, right):
        pl.semaphore_signal(barrier, inc=1, device_id={"tp": neighbour}, device_id_type=MESH)
    mbuf[...] = jnp.full(mbuf.shape, -jnp.inf, jnp.float32)
    acc[...] = jnp.zeros(acc.shape, jnp.float32)
    vbuf[:, :, HD:] = jnp.ones((vbuf.shape[0], rows, HD), jnp.bfloat16)
    pl.semaphore_wait(barrier, peers + 3)

    targets = {1: chip(y + out_dir), 3: chip(y + 3 * out_dir), 2: chip(y - 2 * out_dir)}
    pending = []

    def q_rows(core, h):
        return q_hbm.at[pl.ds(pl.multiple_of(core * half, half), half), pl.ds(pl.multiple_of(h * HD, HD), HD)]

    def q_slot(block):
        return qbuf.at[block, pl.ds(pl.multiple_of(c * half, half), half), :]

    pending.append(send(q_rows(1 - c, head), q_slot(0), q_send.at[0, 0], qsem.at[0, c], twin))
    pending.append(send(head_cols(k_hbm, head), k_at(me), rel_send.at[0, 0], ksem.at[me], twin))
    pending.append(send(head_cols(v_hbm, head), v_at(me), rel_send.at[0, 1], vsem.at[me], twin))
    for k in (3, 2, 1):
        chip_k = targets[k]
        for core in range(2):
            pending.append(
                send(q_rows(core, chip_k // 2), q_slot(k), q_send.at[k, core], qsem.at[k, c], chip_k * 2 + core)
            )
    for k in (2, 3, 1):
        chip_k = targets[k]
        pending.append(send(head_cols(k_hbm, chip_k // 2), k_at(me), kv_send.at[k, 0], ksem.at[me], chip_k * 2 + c))
        pending.append(send(head_cols(v_hbm, chip_k // 2), v_at(me), kv_send.at[k, 1], vsem.at[me], chip_k * 2 + c))
        if k == 2:
            pending.append(send(head_cols(k_hbm, head), k_at(me), kv_send.at[0, 0], ksem.at[me], mate))
            pending.append(send(head_cols(v_hbm, head), v_at(me), kv_send.at[0, 1], vsem.at[me], mate))
    for copy in pending:
        copy.start()

    def forwards(k):
        slot = chip(y + out_dir * k) * 2 + c
        return (
            send(k_at(slot), k_at(slot), fwd_send.at[k, 0], ksem.at[slot], mate),
            send(v_at(slot), v_at(slot), fwd_send.at[k, 1], vsem.at[slot], mate),
            send(k_at(slot), k_at(slot), fwd_send.at[k, 2], ksem.at[slot], twin),
            send(v_at(slot), v_at(slot), fwd_send.at[k, 3], vsem.at[slot], twin),
        )

    def relays(k):
        slot = chip(mate_chip - out_dir * k) * 2 + c
        return (
            send(k_at(slot), k_at(slot), rel_send.at[k + 1, 0], ksem.at[slot], twin),
            send(v_at(slot), v_at(slot), rel_send.at[k + 1, 1], vsem.at[slot], twin),
        )

    def pull_entry(k):
        await_kv(chip(y + out_dir * k) * 2 + c)
        for copy in forwards(k):
            copy.start()

    def pull_mate(k):
        await_kv(chip(mate_chip - out_dir * k) * 2 + c)
        for copy in relays(k):
            copy.start()

    def update(i, key_chip, diagonal):
        keys = kbuf[pl.ds(2 * key_chip, 2)].reshape(2 * rows, HD)
        vals = vbuf[pl.ds(2 * key_chip, 2)].reshape(2 * rows, 2 * HD)
        scores = lax.dot_general(
            qbuf[i], keys, (((1,), (1,)), ((), ())), preferred_element_type=jnp.float32
        )
        if diagonal:
            r = lax.broadcasted_iota(jnp.int32, scores.shape, 0)
            at = jnp.where(r >= half, r - half + rows, r) + c * half
            scores = jnp.where(lax.broadcasted_iota(jnp.int32, scores.shape, 1) <= at, scores, -jnp.inf)
        before = mbuf[i]
        now = jnp.maximum(before, jnp.max(scores, axis=1, keepdims=True))
        mbuf[i] = now
        decay = jnp.exp2((before - now) * factor)
        wide = jnp.concatenate([now] * (2 * rows // HD), axis=1) if 2 * rows > HD else now[:, : 2 * rows]
        weights = jnp.exp2((scores - wide) * factor).astype(jnp.bfloat16)
        acc[i] = acc[i] * jnp.concatenate([decay, decay], axis=1) + jnp.dot(
            weights, vals, preferred_element_type=jnp.float32
        )

    def attend(key_chip):
        def one(i, _):
            query_chip = chip(y + out_dir * i)

            @pl.when(query_chip > key_chip)
            def _():
                update(i, key_chip, False)

            @pl.when(query_chip == key_chip)
            def _():
                update(i, key_chip, True)

            return 0

        lax.fori_loop(0, 4, one, 0)

    pull_mate(0)
    for copy in own:
        copy.wait()
    send(q_slot(0), qbuf.at[0, pl.ds(pl.multiple_of((1 - c) * half, half), half), :], local_sem.at[0],
         qsem.at[0, 1 - c], twin).wait_recv()
    for k in (1, 2, 3):
        for core in range(2):
            send(q_slot(k), qbuf.at[k, pl.ds(core * half, half), :], local_sem.at[0], qsem.at[k, core], twin).wait_recv()

    def stage(k, _):
        @pl.when(k < 4)
        def _():
            pull_entry(k)

        key_chip = chip(y + out_dir * (k - 1))
        await_kv(key_chip * 2 + 1 - c)
        attend(key_chip)

        @pl.when(k < 4)
        def _():
            pull_mate(k)

        key_chip = chip(mate_chip - out_dir * (k - 1))
        await_kv(key_chip * 2 + 1 - c)
        attend(key_chip)
        return 0

    lax.fori_loop(1, 5, stage, 0)

    my_rows = pl.ds(pl.multiple_of(c * half, half), half)

    def finish(i):
        obuf[i] = (acc[i, :, :HD] / acc[i, :, HD:]).astype(jnp.bfloat16)

    back = []
    for i in (3, 2, 1):
        finish(i)
        for core in range(2):
            back.append(
                send(obuf.at[i, pl.ds(core * half, half), :], abuf.at[head, my_rows, :], o_send.at[i, core],
                     asem.at[head, c], chip(y + out_dir * i) * 2 + core)
            )
            back[-1].start()
    finish(0)
    back.append(
        send(obuf.at[0, pl.ds(pl.multiple_of((1 - c) * half, half), half), :], abuf.at[head, my_rows, :],
             o_send.at[0, 0], asem.at[head, c], twin)
    )
    back[-1].start()
    abuf[head, my_rows, :] = obuf[0, my_rows, :]

    kinds = jnp.broadcast_to(mod_ref[...].astype(jnp.float32), (HD, rows)).T
    image = kinds > 0.5
    w_copy.wait()
    for other in range(4):
        for core in range(2):
            @pl.when(jnp.logical_or(head != other, c != core))
            def _():
                send(abuf.at[other, pl.ds(core * half, half), :], abuf.at[other, pl.ds(core * half, half), :],
                     local_sem.at[0], asem.at[other, core], twin).wait_recv()
    for other in range(4):
        piece = abuf[other]
        zero = jnp.zeros_like(piece)
        acat[:, other * HD : (other + 1) * HD] = jnp.where(image, zero, piece)
        acat[:, (other + 4) * HD : (other + 5) * HD] = jnp.where(image, piece, zero)

    def project(step):
        block = lax.rem(z + step + N_TP, N_TP)
        psum[step % N_TP] = jnp.dot(
            acat[...], wbuf[:, pl.ds(pl.multiple_of(block * cols, cols), cols)], preferred_element_type=jnp.float32
        )

    near = (right, left)
    parts = (4, 3, 3, 2, 2, 1, 1)

    def part_rows(way, m):
        low = (m % 2 == 0) == (way == 0)
        return pl.ds(0 if low else half, half)

    def ring_copy(way, m):
        return pltpu.make_async_remote_copy(
            src_ref=rsnd.at[way, m], dst_ref=rrcv.at[way, m], send_sem=r_send.at[way, m], recv_sem=rsem.at[way, m],
            device_id={"tp": near[way]}, device_id_type=MESH,
        )

    def own_part(way, m):
        step = parts[m] if way == 0 else N_TP - parts[m]
        return psum[step % N_TP, part_rows(way, m), :]

    project(4)
    for way in range(2):
        rsnd[way, 0] = own_part(way, 0).astype(jnp.bfloat16)
        ring_copy(way, 0).start()
    for way in range(2):
        project(3 - 6 * way)
        rsnd[way, 1] = own_part(way, 1).astype(jnp.bfloat16)
        ring_copy(way, 1).start()
    for step in (2, -2, 1, -1, 0):
        project(step)
    for m in range(2, 7):
        for way in range(2):
            ring_copy(way, m - 2).wait_recv()
            rsnd[way, m] = (own_part(way, m) + rrcv[way, m - 2].astype(jnp.float32)).astype(jnp.bfloat16)
            ring_copy(way, m).start()
    for way in range(2):
        for m in (5, 6):
            ring_copy(way, m).wait_recv()
    for low, (a, b) in enumerate(((5, 6), (6, 5))):
        span = pl.ds(0 if low else half, half)
        out_ref[span, :] = (
            psum[0, span, :] + rrcv[0, a].astype(jnp.float32) + rrcv[1, b].astype(jnp.float32)
        ).astype(jnp.bfloat16)

    for copy in pending + back:
        copy.wait_send()
    for k in (1, 2, 3):
        for copy in forwards(k):
            copy.wait_send()
    for k in (0, 1, 2, 3):
        for copy in relays(k):
            copy.wait_send()
    for way in range(2):
        for m in range(7):
            ring_copy(way, m).wait_send()


def on_device(queries, key_rows, values, modality, out_weight):
    rows, width = queries.shape
    cols = out_weight.shape[2] // N_TP
    half = rows // 2
    bf, f32 = jnp.bfloat16, jnp.float32
    dma = pltpu.SemaphoreType.DMA
    anywhere = pl.BlockSpec(memory_space=pl.ANY)
    vmem = pl.BlockSpec(memory_space=pltpu.VMEM)
    return pl.pallas_call(
        fused,
        out_shape=jax.ShapeDtypeStruct((rows, cols), bf),
        in_specs=[anywhere, anywhere, anywhere, vmem, anywhere],
        out_specs=vmem,
        scratch_shapes=[
            pltpu.VMEM((4, rows, HD), bf),
            pltpu.VMEM((16, rows, HD), bf),
            pltpu.VMEM((16, rows, 2 * HD), bf),
            pltpu.VMEM((4, rows, HD), f32),
            pltpu.VMEM((4, rows, 2 * HD), f32),
            pltpu.VMEM((4, rows, HD), bf),
            pltpu.VMEM((4, rows, HD), bf),
            pltpu.VMEM((rows, 2 * width), bf),
            pltpu.VMEM((2 * width, out_weight.shape[2]), bf),
            pltpu.VMEM((N_TP, rows, cols), f32),
            pltpu.VMEM((2, 7, half, cols), bf),
            pltpu.VMEM((2, 7, half, cols), bf),
            dma((2,)), dma((16,)), dma((16,)), dma((4, 2)), dma((4, 2)), dma((2, 7)),
            dma((4, 2)), dma((4, 2)), dma((4, 4)), dma((5, 2)), dma((4, 2)), dma((2, 7)),
        ],
        compiler_params=pltpu.CompilerParams(
            collective_id=0, has_side_effects=True, vmem_limit_bytes=56 * 1024 * 1024
        ),
    )(queries, key_rows, values, modality.reshape(1, rows), out_weight.reshape(2 * width, out_weight.shape[2]))


def solution(mesh):
    in_specs = (
        P(("dp", "seq"), "tp"),
        P(("dp", "seq"), "tp"),
        P(("dp", "seq"), "tp"),
        P(("dp", "seq")),
        P(None, "tp", None),
    )
    out_specs = P(("dp", "seq"), "tp")
    return jax.shard_map(
        on_device, mesh=mesh, in_specs=in_specs, out_specs=out_specs, check_vma=False
    )
```

```python
import jax
import jax.numpy as jnp
from jax import lax
from jax.experimental import pallas as pl
from jax.experimental.pallas import tpu as pltpu
from jax.sharding import PartitionSpec as P

HD = 128
N_TP = 8
MESH = pl.DeviceIdType.MESH
LOG2E = 1.4426950408889634
CH = 2


def fused(
    q_hbm, k_hbm, v_hbm, mod_ref, w_hbm, out_ref,
    qbuf, kbuf, vbuf, mbuf, acc, obuf, abuf, image, acat, wbuf, psum, rsnd, rrcv,
    local_sem, ksem, vsem, qsem, asem, rsem, q_send, kv_send, fwd_send, rel_send, o_send, r_send,
):
    me = lax.axis_index("seq")
    z = lax.axis_index("tp")
    rows = q_hbm.shape[0]
    half = rows // 2
    cols = out_ref.shape[1]
    y = me // 2
    c = me % 2
    side = y % 2
    out_dir = 2 * side - 1
    head = y // 2
    twin = 1 - 2 * c + me
    mate_chip = y - out_dir
    mate = mate_chip * 2 + c
    factor = HD ** (-0.5) * LOG2E

    def chip(t):
        return lax.rem(t + 16, 8)

    def send(src, dst, ssem, rsem_, seq):
        copy = pltpu.make_async_remote_copy(
            src_ref=src, dst_ref=dst, send_sem=ssem, recv_sem=rsem_,
            device_id={"seq": seq}, device_id_type=MESH,
        )
        return copy

    def k_at(slot):
        return kbuf.at[slot]

    def v_at(slot):
        return vbuf.at[slot, :, pl.ds(0, HD)]

    def head_cols(ref, h):
        return ref.at[:, pl.ds(pl.multiple_of(h * HD, HD), HD)]

    def await_kv(slot):
        send(k_at(slot), k_at(slot), local_sem.at[0], ksem.at[slot], twin).wait_recv()
        send(v_at(slot), v_at(slot), local_sem.at[0], vsem.at[slot], twin).wait_recv()

    own = [
        pltpu.make_async_copy(head_cols(k_hbm, head), k_at(me), ksem.at[me]),
        pltpu.make_async_copy(head_cols(v_hbm, head), v_at(me), vsem.at[me]),
        pltpu.make_async_copy(
            q_hbm.at[pl.ds(pl.multiple_of(c * half, half), half), pl.ds(pl.multiple_of(head * HD, HD), HD)],
            qbuf.at[0, pl.ds(pl.multiple_of(c * half, half), half), :],
            qsem.at[0, c],
        ),
    ]
    for copy in own:
        copy.start()
    w_copy = pltpu.make_async_copy(w_hbm, wbuf, local_sem.at[1])
    w_copy.start()

    barrier = pltpu.get_barrier_semaphore()
    left, right = lax.rem(z + N_TP - 1, N_TP), lax.rem(z + 1, N_TP)
    peers = 0
    for step in (1, 2, 3, -1, -2):
        for core in range(2):
            pl.semaphore_signal(
                barrier, inc=1, device_id={"seq": chip(y + out_dir * step) * 2 + core}, device_id_type=MESH
            )
            peers += 1
    pl.semaphore_signal(barrier, inc=1, device_id={"seq": twin}, device_id_type=MESH)
    for neighbour in (left, right):
        pl.semaphore_signal(barrier, inc=1, device_id={"tp": neighbour}, device_id_type=MESH)
    mbuf[...] = jnp.full(mbuf.shape, -jnp.inf, jnp.float32)
    acc[...] = jnp.zeros(acc.shape, jnp.float32)
    vbuf[:, :, HD:] = jnp.ones((vbuf.shape[0], rows, HD), jnp.bfloat16)
    pl.semaphore_wait(barrier, peers + 3)

    targets = {1: chip(y + out_dir), 3: chip(y + 3 * out_dir), 2: chip(y - 2 * out_dir)}
    pending = []

    def q_rows(core, h):
        return q_hbm.at[pl.ds(pl.multiple_of(core * half, half), half), pl.ds(pl.multiple_of(h * HD, HD), HD)]

    def q_slot(block):
        return qbuf.at[block, pl.ds(pl.multiple_of(c * half, half), half), :]

    pending.append(send(q_rows(1 - c, head), q_slot(0), q_send.at[0, 0], qsem.at[0, c], twin))
    pending.append(send(head_cols(k_hbm, head), k_at(me), rel_send.at[0, 0], ksem.at[me], twin))
    pending.append(send(head_cols(v_hbm, head), v_at(me), rel_send.at[0, 1], vsem.at[me], twin))

    def add_q(k):
        chip_k = targets[k]
        for core in range(2):
            pending.append(
                send(q_rows(core, chip_k // 2), q_slot(k), q_send.at[k, core], qsem.at[k, c], chip_k * 2 + core)
            )

    def add_kv(k):
        chip_k = targets[k] if k else mate_chip
        seq = mate if k == 0 else chip_k * 2 + c
        pending.append(send(head_cols(k_hbm, chip_k // 2), k_at(me), kv_send.at[k, 0], ksem.at[me], seq))
        pending.append(send(head_cols(v_hbm, chip_k // 2), v_at(me), kv_send.at[k, 1], vsem.at[me], seq))

    add_kv(1), add_kv(2), add_kv(3), add_kv(0), add_q(1), add_q(2), add_q(3)
    for copy in pending:
        copy.start()

    def forwards(k):
        slot = chip(y + out_dir * k) * 2 + c
        return (
            send(k_at(slot), k_at(slot), fwd_send.at[k, 0], ksem.at[slot], mate),
            send(v_at(slot), v_at(slot), fwd_send.at[k, 1], vsem.at[slot], mate),
            send(k_at(slot), k_at(slot), fwd_send.at[k, 2], ksem.at[slot], twin),
            send(v_at(slot), v_at(slot), fwd_send.at[k, 3], vsem.at[slot], twin),
        )

    def relays(k):
        slot = chip(mate_chip - out_dir * k) * 2 + c
        return (
            send(k_at(slot), k_at(slot), rel_send.at[k + 1, 0], ksem.at[slot], twin),
            send(v_at(slot), v_at(slot), rel_send.at[k + 1, 1], vsem.at[slot], twin),
        )

    def pull_entry(k):
        await_kv(chip(y + out_dir * k) * 2 + c)
        for copy in forwards(k):
            copy.start()

    def pull_mate(k):
        await_kv(chip(mate_chip - out_dir * k) * 2 + c)
        for copy in relays(k):
            copy.start()

    def update(i, key_chip, diagonal):
        keys = kbuf[pl.ds(2 * key_chip, 2)].reshape(2 * rows, HD)
        vals = vbuf[pl.ds(2 * key_chip, 2)].reshape(2 * rows, 2 * HD)
        scores = lax.dot_general(
            qbuf[i], keys, (((1,), (1,)), ((), ())), preferred_element_type=jnp.float32
        )
        if diagonal:
            r = lax.broadcasted_iota(jnp.int32, scores.shape, 0)
            at = jnp.where(r >= half, r - half + rows, r) + c * half
            scores = jnp.where(lax.broadcasted_iota(jnp.int32, scores.shape, 1) <= at, scores, -jnp.inf)
        before = mbuf[i]
        now = jnp.maximum(before, jnp.max(scores, axis=1, keepdims=True))
        mbuf[i] = now
        decay = jnp.exp2((before - now) * factor)
        wide = jnp.concatenate([now] * (2 * rows // HD), axis=1) if 2 * rows > HD else now[:, : 2 * rows]
        weights = jnp.exp2((scores - wide) * factor).astype(jnp.bfloat16)
        acc[i] = acc[i] * jnp.concatenate([decay, decay], axis=1) + jnp.dot(
            weights, vals, preferred_element_type=jnp.float32
        )

    def attend(key_chip):
        def one(i, _):
            query_chip = chip(y + out_dir * i)

            @pl.when(query_chip > key_chip)
            def _():
                update(i, key_chip, False)

            @pl.when(query_chip == key_chip)
            def _():
                update(i, key_chip, True)

            return 0

        lax.fori_loop(0, 4, one, 0)

    def attend_events(first, last):
        def one(event, _):
            key_chip = chip(jnp.where(event < 4, y + out_dir * event, mate_chip - out_dir * (event - 4)))
            await_kv(key_chip * 2 + 1 - c)
            attend(key_chip)
            return 0

        lax.fori_loop(first, last, one, 0)

    def await_q():
        for copy in own:
            copy.wait()
        send(q_slot(0), qbuf.at[0, pl.ds(pl.multiple_of((1 - c) * half, half), half), :], local_sem.at[0],
             qsem.at[0, 1 - c], twin).wait_recv()
        for k in (1, 2, 3):
            for core in range(2):
                send(q_slot(k), qbuf.at[k, pl.ds(core * half, half), :], local_sem.at[0], qsem.at[k, core],
                     twin).wait_recv()

    pull_entry(1), pull_entry(2), pull_entry(3), pull_mate(0)
    await_q()
    attend_events(0, 2)
    pull_mate(1)
    attend_events(2, 5)
    pull_mate(2)
    attend_events(5, 6)
    pull_mate(3)
    attend_events(6, 8)

    part = half // CH
    back = []

    def give_back(r):
        at = pl.ds(pl.multiple_of(c * half + r * part, part), part)
        for i in (3, 2, 1, 0):
            for core in range(2):
                span = pl.ds(core * half + r * part, part)
                obuf[i, span, :] = (acc[i, span, :HD] / acc[i, span, HD:]).astype(jnp.bfloat16)
        for i in (3, 2, 1):
            for core in range(2):
                back.append(
                    send(obuf.at[i, pl.ds(core * half + r * part, part), :], abuf.at[head, at, :],
                         o_send.at[r, i, core], asem.at[r, head, c], chip(y + out_dir * i) * 2 + core)
                )
                back[-1].start()
        back.append(
            send(obuf.at[0, pl.ds(pl.multiple_of((1 - c) * half + r * part, part), part), :], abuf.at[head, at, :],
                 o_send.at[r, 0, 0], asem.at[r, head, c], twin)
        )
        back[-1].start()
        abuf[head, at, :] = obuf[0, at, :]

    kinds = jnp.broadcast_to(mod_ref[...].astype(jnp.float32), (HD, rows)).T
    image[...] = kinds
    for r in range(CH):
        give_back(r)
    w_copy.wait()

    def receive(r):
        for other in range(4):
            for core in range(2):
                @pl.when(jnp.logical_or(head != other, c != core))
                def _():
                    landed = abuf.at[other, pl.ds(core * half + r * part, part), :]
                    send(landed, landed, local_sem.at[0], asem.at[r, other, core], twin).wait_recv()
        for other in range(4):
            for core in range(2):
                span = pl.ds(core * half + r * part, part)
                piece = abuf[other, span, :]
                zero = jnp.zeros_like(piece)
                chosen = image[span, :] > 0.5
                to = pl.ds(core * part, part)
                acat[r, to, other * HD : (other + 1) * HD] = jnp.where(chosen, zero, piece)
                acat[r, to, (other + 4) * HD : (other + 5) * HD] = jnp.where(chosen, piece, zero)

    def project(r, step):
        block = lax.rem(z + step + N_TP, N_TP)
        psum[r, step % N_TP] = jnp.dot(
            acat[r], wbuf[:, pl.ds(pl.multiple_of(block * cols, cols), cols)], preferred_element_type=jnp.float32
        )

    near = (right, left)
    parts = (4, 3, 3, 2, 2, 1, 1)

    def ring_copy(r, way, m):
        return pltpu.make_async_remote_copy(
            src_ref=rsnd.at[r, way, m], dst_ref=rrcv.at[r, way, m], send_sem=r_send.at[r, way, m],
            recv_sem=rsem.at[r, way, m], device_id={"tp": near[way]}, device_id_type=MESH,
        )

    def own_part(r, way, m):
        step = parts[m] if way == 0 else N_TP - parts[m]
        low = (m % 2 == 0) == (way == 0)
        return psum[r, step % N_TP, pl.ds(0 if low else part, part), :]

    def ring_open(r):
        receive(r)
        project(r, 4)
        for way in range(2):
            rsnd[r, way, 0] = own_part(r, way, 0).astype(jnp.bfloat16)
            ring_copy(r, way, 0).start()
        for way in range(2):
            project(r, 3 - 6 * way)
            rsnd[r, way, 1] = own_part(r, way, 1).astype(jnp.bfloat16)
            ring_copy(r, way, 1).start()
        for step in (2, -2, 1, -1, 0):
            project(r, step)

    def ring_step(r, m):
        for way in range(2):
            ring_copy(r, way, m - 2).wait_recv()
            rsnd[r, way, m] = (own_part(r, way, m) + rrcv[r, way, m - 2].astype(jnp.float32)).astype(jnp.bfloat16)
            ring_copy(r, way, m).start()

    def ring_close(r):
        for way in range(2):
            for m in (5, 6):
                ring_copy(r, way, m).wait_recv()
        for core, (a, b) in enumerate(((6, 5), (5, 6))):
            out_ref[pl.ds(core * half + r * part, part), :] = (
                psum[r, 0, pl.ds(core * part, part), :]
                + rrcv[r, 0, a].astype(jnp.float32)
                + rrcv[r, 1, b].astype(jnp.float32)
            ).astype(out_ref.dtype)

    for slot in range(CH + 6):
        for r in reversed(range(CH)):
            phase = slot - r
            if phase == 0:
                ring_open(r)
            elif 1 <= phase <= 5:
                ring_step(r, phase + 1)
            elif phase == 6:
                ring_close(r)

    for copy in pending + back:
        copy.wait_send()
    for k in (1, 2, 3):
        for copy in forwards(k):
            copy.wait_send()
    for k in (0, 1, 2, 3):
        for copy in relays(k):
            copy.wait_send()
    for r in range(CH):
        for way in range(2):
            for m in range(7):
                ring_copy(r, way, m).wait_send()


def on_device(queries, key_rows, values, modality, out_weight):
    rows, width = queries.shape
    cols = out_weight.shape[2] // N_TP
    half = rows // 2
    bf, f32 = jnp.bfloat16, jnp.float32
    dma = pltpu.SemaphoreType.DMA
    anywhere = pl.BlockSpec(memory_space=pl.ANY)
    vmem = pl.BlockSpec(memory_space=pltpu.VMEM)
    return pl.pallas_call(
        fused,
        out_shape=jax.ShapeDtypeStruct((rows, cols), f32),
        in_specs=[anywhere, anywhere, anywhere, vmem, anywhere],
        out_specs=vmem,
        scratch_shapes=[
            pltpu.VMEM((4, rows, HD), bf),
            pltpu.VMEM((16, rows, HD), bf),
            pltpu.VMEM((16, rows, 2 * HD), bf),
            pltpu.VMEM((4, rows, HD), f32),
            pltpu.VMEM((4, rows, 2 * HD), f32),
            pltpu.VMEM((4, rows, HD), bf),
            pltpu.VMEM((4, rows, HD), bf),
            pltpu.VMEM((rows, HD), f32),
            pltpu.VMEM((CH, rows // CH, 2 * width), bf),
            pltpu.VMEM((2 * width, out_weight.shape[2]), bf),
            pltpu.VMEM((CH, N_TP, rows // CH, cols), f32),
            pltpu.VMEM((CH, 2, 7, half // CH, cols), bf),
            pltpu.VMEM((CH, 2, 7, half // CH, cols), bf),
            dma((2,)), dma((16,)), dma((16,)), dma((4, 2)), dma((CH, 4, 2)), dma((CH, 2, 7)),
            dma((4, 2)), dma((4, 2)), dma((4, 4)), dma((5, 2)), dma((CH, 4, 2)), dma((CH, 2, 7)),
        ],
        compiler_params=pltpu.CompilerParams(
            collective_id=0, has_side_effects=True, vmem_limit_bytes=56 * 1024 * 1024
        ),
    )(queries, key_rows, values, modality.reshape(1, rows), out_weight.reshape(2 * width, out_weight.shape[2])).astype(bf)


def solution(mesh):
    in_specs = (
        P(("dp", "seq"), "tp"),
        P(("dp", "seq"), "tp"),
        P(("dp", "seq"), "tp"),
        P(("dp", "seq")),
        P(None, "tp", None),
    )
    out_specs = P(("dp", "seq"), "tp")
    return jax.shard_map(
        on_device, mesh=mesh, in_specs=in_specs, out_specs=out_specs, check_vma=False
    )
```

```python
import jax
import jax.numpy as jnp
from jax import lax
from jax.experimental import pallas as pl
from jax.experimental.pallas import tpu as pltpu
from jax.sharding import PartitionSpec as P

HD = 128
N_TP = 8
MESH = pl.DeviceIdType.MESH
LOG2E = 1.4426950408889634
CH = 2
PLAN = (
    ("E", 1), ("E", 2), ("Q",), ("A", 0, 1), ("E", 3), ("M", 0), ("A", 1, 3), ("M", 1), ("A", 3, 5), ("M", 2), ("A", 5, 6),
    ("M", 3), ("A", 6, 8),
)


def fused(
    q_hbm, k_hbm, v_hbm, mod_ref, w_hbm, out_ref,
    qbuf, kbuf, vbuf, mbuf, lbuf, vt, acc, obuf, abuf, image, acat, wbuf, psum, rsnd, rrcv,
    local_sem, ksem, vsem, qsem, asem, rsem, q_send, kv_send, fwd_send, rel_send, o_send, r_send,
):
    me = lax.axis_index("seq")
    z = lax.axis_index("tp")
    rows = q_hbm.shape[0]
    half = rows // 2
    cols = out_ref.shape[1]
    y = me // 2
    c = me % 2
    side = y % 2
    out_dir = 2 * side - 1
    head = y // 2
    twin = 1 - 2 * c + me
    mate_chip = y - out_dir
    mate = mate_chip * 2 + c
    factor = HD ** (-0.5) * LOG2E

    def chip(t):
        return lax.rem(t + 16, 8)

    def send(src, dst, ssem, rsem_, seq):
        copy = pltpu.make_async_remote_copy(
            src_ref=src, dst_ref=dst, send_sem=ssem, recv_sem=rsem_,
            device_id={"seq": seq}, device_id_type=MESH,
        )
        return copy

    def k_at(slot):
        return kbuf.at[slot]

    def v_at(slot):
        return vbuf.at[slot]

    def head_cols(ref, h):
        return ref.at[:, pl.ds(pl.multiple_of(h * HD, HD), HD)]

    def await_kv(slot):
        send(k_at(slot), k_at(slot), local_sem.at[0], ksem.at[slot], twin).wait_recv()
        send(v_at(slot), v_at(slot), local_sem.at[0], vsem.at[slot], twin).wait_recv()

    own = [
        pltpu.make_async_copy(head_cols(k_hbm, head), k_at(me), ksem.at[me]),
        pltpu.make_async_copy(head_cols(v_hbm, head), v_at(me), vsem.at[me]),
        pltpu.make_async_copy(
            q_hbm.at[pl.ds(pl.multiple_of(c * half, half), half), pl.ds(pl.multiple_of(head * HD, HD), HD)],
            qbuf.at[0, pl.ds(pl.multiple_of(c * half, half), half), :],
            qsem.at[0, c],
        ),
    ]
    for copy in own:
        copy.start()
    w_copy = pltpu.make_async_copy(w_hbm, wbuf, local_sem.at[1])
    w_copy.start()

    barrier = pltpu.get_barrier_semaphore()
    left, right = lax.rem(z + N_TP - 1, N_TP), lax.rem(z + 1, N_TP)
    peers = 0
    for step in (1, 2, 3, -1, -2):
        for core in range(2):
            pl.semaphore_signal(
                barrier, inc=1, device_id={"seq": chip(y + out_dir * step) * 2 + core}, device_id_type=MESH
            )
            peers += 1
    pl.semaphore_signal(barrier, inc=1, device_id={"seq": twin}, device_id_type=MESH)
    for neighbour in (left, right):
        pl.semaphore_signal(barrier, inc=1, device_id={"tp": neighbour}, device_id_type=MESH)
    mbuf[...] = jnp.full(mbuf.shape, -jnp.inf, jnp.float32)
    acc[...] = jnp.zeros(acc.shape, jnp.float32)
    lbuf[...] = jnp.zeros(lbuf.shape, jnp.float32)
    pl.semaphore_wait(barrier, peers + 3)

    targets = {1: chip(y + out_dir), 3: chip(y + 3 * out_dir), 2: chip(y - 2 * out_dir)}
    pending = []

    def q_rows(core, h):
        return q_hbm.at[pl.ds(pl.multiple_of(core * half, half), half), pl.ds(pl.multiple_of(h * HD, HD), HD)]

    def q_slot(block):
        return qbuf.at[block, pl.ds(pl.multiple_of(c * half, half), half), :]

    pending.append(send(q_rows(1 - c, head), q_slot(0), q_send.at[0, 0], qsem.at[0, c], twin))
    pending.append(send(head_cols(k_hbm, head), k_at(me), rel_send.at[0, 0], ksem.at[me], twin))
    pending.append(send(head_cols(v_hbm, head), v_at(me), rel_send.at[0, 1], vsem.at[me], twin))

    def add_q(k):
        chip_k = targets[k]
        for core in range(2):
            pending.append(
                send(q_rows(core, chip_k // 2), q_slot(k), q_send.at[k, core], qsem.at[k, c], chip_k * 2 + core)
            )

    def add_kv(k):
        chip_k = targets[k] if k else mate_chip
        seq = mate if k == 0 else chip_k * 2 + c
        pending.append(send(head_cols(k_hbm, chip_k // 2), k_at(me), kv_send.at[k, 0], ksem.at[me], seq))
        pending.append(send(head_cols(v_hbm, chip_k // 2), v_at(me), kv_send.at[k, 1], vsem.at[me], seq))

    add_kv(1), add_kv(2), add_q(1), add_q(3), add_q(2), add_kv(3), add_kv(0)
    for copy in pending:
        copy.start()

    def forwards(k):
        slot = chip(y + out_dir * k) * 2 + c
        return (
            send(k_at(slot), k_at(slot), fwd_send.at[k, 0], ksem.at[slot], mate),
            send(v_at(slot), v_at(slot), fwd_send.at[k, 1], vsem.at[slot], mate),
            send(k_at(slot), k_at(slot), fwd_send.at[k, 2], ksem.at[slot], twin),
            send(v_at(slot), v_at(slot), fwd_send.at[k, 3], vsem.at[slot], twin),
        )

    def relays(k):
        slot = chip(mate_chip - out_dir * k) * 2 + c
        return (
            send(k_at(slot), k_at(slot), rel_send.at[k + 1, 0], ksem.at[slot], twin),
            send(v_at(slot), v_at(slot), rel_send.at[k + 1, 1], vsem.at[slot], twin),
        )

    def pull_entry(k):
        await_kv(chip(y + out_dir * k) * 2 + c)
        for copy in forwards(k):
            copy.start()

    def pull_mate(k):
        await_kv(chip(mate_chip - out_dir * k) * 2 + c)
        for copy in relays(k):
            copy.start()

    def update(blocks, key_chip, diagonal):
        keys = kbuf[pl.ds(2 * key_chip, 2)].reshape(2 * rows, HD)
        scores = [
            lax.dot_general(keys, qbuf[i], (((1,), (1,)), ((), ())), preferred_element_type=jnp.float32)
            for i in blocks
        ]
        if diagonal:
            q = lax.broadcasted_iota(jnp.int32, scores[0].shape, 1)
            at = jnp.where(q >= half, q - half + rows, q) + c * half
            seen = lax.broadcasted_iota(jnp.int32, scores[0].shape, 0) <= at
            scores = [jnp.where(seen, s, -jnp.inf) for s in scores]
        state = [(mbuf[i], lbuf[i], acc[i]) for i in blocks]
        fresh = []
        for s, (top, total, sums) in zip(scores, state):
            now = jnp.maximum(top, jnp.max(s, axis=0, keepdims=True))
            decay = jnp.exp2((top - now) * factor)
            weights = jnp.exp2((s - now) * factor)
            total = total * decay + jnp.sum(weights, axis=0, keepdims=True)
            sums = sums * decay + jnp.dot(
                vt[...], weights.astype(jnp.bfloat16), preferred_element_type=jnp.float32
            )
            fresh.append((now, total, sums))
        for i, (now, total, sums) in zip(blocks, fresh):
            mbuf[i], lbuf[i], acc[i] = now, total, sums

    def attend(key_chip):
        vt[...] = vbuf[pl.ds(2 * key_chip, 2)].reshape(2 * rows, HD).T

        def one(i):
            query_chip = chip(y + out_dir * i)

            @pl.when(query_chip > key_chip)
            def _():
                update((i,), key_chip, False)

            @pl.when(query_chip == key_chip)
            def _():
                update((i,), key_chip, True)

        def pair(j, _):
            first, second = 2 * j + 1, lax.rem(2 * j + 2, 4)
            lower = jnp.minimum(chip(y + out_dir * first), chip(y + out_dir * second))

            @pl.when(lower > key_chip)
            def _():
                update((first, second), key_chip, False)

            @pl.when(lower <= key_chip)
            def _():
                def each(t, _):
                    one(jnp.where(t == 0, first, second))
                    return 0

                lax.fori_loop(0, 2, each, 0)

            return 0

        lax.fori_loop(0, 2, pair, 0)

    def attend_events(first, last):
        def one(event, _):
            key_chip = chip(jnp.where(event < 4, y + out_dir * event, mate_chip - out_dir * (event - 4)))
            await_kv(key_chip * 2 + 1 - c)
            attend(key_chip)
            return 0

        lax.fori_loop(first, last, one, 0)

    def await_q():
        for copy in own:
            copy.wait()
        send(q_slot(0), qbuf.at[0, pl.ds(pl.multiple_of((1 - c) * half, half), half), :], local_sem.at[0],
             qsem.at[0, 1 - c], twin).wait_recv()
        for k in (1, 2, 3):
            for core in range(2):
                send(q_slot(k), qbuf.at[k, pl.ds(core * half, half), :], local_sem.at[0], qsem.at[k, core],
                     twin).wait_recv()

    for kind, *span in PLAN:
        {"E": pull_entry, "M": pull_mate, "Q": await_q, "A": attend_events}[kind](*span)

    part = half // CH
    back = []

    def give_back(r):
        at = pl.ds(pl.multiple_of(c * half + r * part, part), part)
        for i in (3, 2, 1):
            for core in range(2):
                back.append(
                    send(obuf.at[i, pl.ds(core * half + r * part, part), :], abuf.at[head, at, :],
                         o_send.at[r, i, core], asem.at[r, head, c], chip(y + out_dir * i) * 2 + core)
                )
                back[-1].start()
        back.append(
            send(obuf.at[0, pl.ds(pl.multiple_of((1 - c) * half + r * part, part), part), :], abuf.at[head, at, :],
                 o_send.at[r, 0, 0], asem.at[r, head, c], twin)
        )
        back[-1].start()
        abuf[head, at, :] = obuf[0, at, :]

    kinds = jnp.broadcast_to(mod_ref[...].astype(jnp.float32), (HD, rows)).T
    image[...] = kinds
    for i in range(4):
        obuf[i] = (acc[i] / lbuf[i]).T.astype(jnp.bfloat16)
    for r in range(CH):
        give_back(r)
    w_copy.wait()

    def receive(r):
        for other in range(4):
            for core in range(2):
                @pl.when(jnp.logical_or(head != other, c != core))
                def _():
                    landed = abuf.at[other, pl.ds(core * half + r * part, part), :]
                    send(landed, landed, local_sem.at[0], asem.at[r, other, core], twin).wait_recv()
        for other in range(4):
            for core in range(2):
                span = pl.ds(core * half + r * part, part)
                piece = abuf[other, span, :]
                zero = jnp.zeros_like(piece)
                chosen = image[span, :] > 0.5
                to = pl.ds(core * part, part)
                acat[r, to, other * HD : (other + 1) * HD] = jnp.where(chosen, zero, piece)
                acat[r, to, (other + 4) * HD : (other + 5) * HD] = jnp.where(chosen, piece, zero)

    def project(r, step):
        block = lax.rem(z + step + N_TP, N_TP)
        psum[r, step % N_TP] = jnp.dot(
            acat[r], wbuf[:, pl.ds(pl.multiple_of(block * cols, cols), cols)], preferred_element_type=jnp.float32
        )

    near = (right, left)
    parts = (4, 3, 3, 2, 2, 1, 1)

    def ring_copy(r, way, m):
        return pltpu.make_async_remote_copy(
            src_ref=rsnd.at[r, way, m], dst_ref=rrcv.at[r, way, m], send_sem=r_send.at[r, way, m],
            recv_sem=rsem.at[r, way, m], device_id={"tp": near[way]}, device_id_type=MESH,
        )

    def own_part(r, way, m):
        step = parts[m] if way == 0 else N_TP - parts[m]
        low = (m % 2 == 0) == (way == 0)
        return psum[r, step % N_TP, pl.ds(0 if low else part, part), :]

    def ring_open(r):
        receive(r)
        project(r, 4)
        for way in range(2):
            rsnd[r, way, 0] = own_part(r, way, 0).astype(jnp.bfloat16)
            ring_copy(r, way, 0).start()
        for way in range(2):
            project(r, 3 - 6 * way)
            rsnd[r, way, 1] = own_part(r, way, 1).astype(jnp.bfloat16)
            ring_copy(r, way, 1).start()

    def ring_step(r, m):
        for way in range(2):
            ring_copy(r, way, m - 2).wait_recv()
            rsnd[r, way, m] = (own_part(r, way, m) + rrcv[r, way, m - 2].astype(jnp.float32)).astype(jnp.bfloat16)
            ring_copy(r, way, m).start()
        for step in {2: (2, -2), 4: (1, -1), 6: (0,)}.get(m, ()):
            project(r, step)

    def ring_close(r):
        for way in range(2):
            for m in (5, 6):
                ring_copy(r, way, m).wait_recv()
        for core, (a, b) in enumerate(((6, 5), (5, 6))):
            out_ref[pl.ds(core * half + r * part, part), :] = (
                psum[r, 0, pl.ds(core * part, part), :]
                + rrcv[r, 0, a].astype(jnp.float32)
                + rrcv[r, 1, b].astype(jnp.float32)
            ).astype(out_ref.dtype)

    for slot in range(CH + 6):
        for r in reversed(range(CH)):
            phase = slot - r
            if phase == 0:
                ring_open(r)
            elif 1 <= phase <= 5:
                ring_step(r, phase + 1)
            elif phase == 6:
                ring_close(r)

    for copy in pending + back:
        copy.wait_send()
    for k in (1, 2, 3):
        for copy in forwards(k):
            copy.wait_send()
    for k in (0, 1, 2, 3):
        for copy in relays(k):
            copy.wait_send()
    for r in range(CH):
        for way in range(2):
            for m in range(7):
                ring_copy(r, way, m).wait_send()


def on_device(queries, key_rows, values, modality, out_weight):
    rows, width = queries.shape
    cols = out_weight.shape[2] // N_TP
    half = rows // 2
    bf, f32 = jnp.bfloat16, jnp.float32
    dma = pltpu.SemaphoreType.DMA
    anywhere = pl.BlockSpec(memory_space=pl.ANY)
    vmem = pl.BlockSpec(memory_space=pltpu.VMEM)
    return pl.pallas_call(
        fused,
        out_shape=jax.ShapeDtypeStruct((rows, cols), f32),
        in_specs=[anywhere, anywhere, anywhere, vmem, anywhere],
        out_specs=vmem,
        scratch_shapes=[
            pltpu.VMEM((4, rows, HD), bf),
            pltpu.VMEM((16, rows, HD), bf),
            pltpu.VMEM((16, rows, HD), bf),
            pltpu.VMEM((4, 1, rows), f32),
            pltpu.VMEM((4, 1, rows), f32),
            pltpu.VMEM((HD, 2 * rows), bf),
            pltpu.VMEM((4, HD, rows), f32),
            pltpu.VMEM((4, rows, HD), bf),
            pltpu.VMEM((4, rows, HD), bf),
            pltpu.VMEM((rows, HD), f32),
            pltpu.VMEM((CH, rows // CH, 2 * width), bf),
            pltpu.VMEM((2 * width, out_weight.shape[2]), bf),
            pltpu.VMEM((CH, N_TP, rows // CH, cols), f32),
            pltpu.VMEM((CH, 2, 7, half // CH, cols), bf),
            pltpu.VMEM((CH, 2, 7, half // CH, cols), bf),
            dma((2,)), dma((16,)), dma((16,)), dma((4, 2)), dma((CH, 4, 2)), dma((CH, 2, 7)),
            dma((4, 2)), dma((4, 2)), dma((4, 4)), dma((5, 2)), dma((CH, 4, 2)), dma((CH, 2, 7)),
        ],
        compiler_params=pltpu.CompilerParams(
            collective_id=0, has_side_effects=True, vmem_limit_bytes=56 * 1024 * 1024
        ),
    )(queries, key_rows, values, modality.reshape(1, rows), out_weight.reshape(2 * width, out_weight.shape[2])).astype(bf)


def solution(mesh):
    in_specs = (
        P(("dp", "seq"), "tp"),
        P(("dp", "seq"), "tp"),
        P(("dp", "seq"), "tp"),
        P(("dp", "seq")),
        P(None, "tp", None),
    )
    out_specs = P(("dp", "seq"), "tp")
    return jax.shard_map(
        on_device, mesh=mesh, in_specs=in_specs, out_specs=out_specs, check_vma=False
    )
```
